32 devices in a mesh: rows: 8 (over z, core), aux: 4 (over y, x).
Axes of the slice: x: 2, y: 2, z: 4, core: 2. Of those that a mesh axis runs over, the one named last changes fastest.
Arguments:
- pair_coeffs: float32 [36000, 8192], P('aux', 'rows'), may hold values from -0.0625 to 0.0625
- pair_gaps: float32 [8192], P('rows'), may hold values from 0.2 to 20
- trial_vectors: float32 [36000, 128], P('aux'), may hold values from -0.03125 to 0.03125
Outputs:
- vectors_out: float32 [36000, 128], P('aux')
- rayleigh: float32 [128, 128], replicated
The draws below stay inside these ranges and needn't reach their ends.
All inputs are finite; a program needn't handle non-finite values.
Results may differ from the reference program's by a relative error of at most 0.00011.
Values sent between devices are 32-bit elements; how exact they have to be, the bound alone decides.
A program may use at most 128 MiB of HBM per device.

```python
import math
import jax
import jax.numpy as jnp
from jax import lax

NAUX = 36000
K = 128
ITERS = 2
PAIRS = 8192


def shard_levels(stream_key, shape, pieces, low, top_value):
    def one(position, shards_of):
        steps = jax.random.uniform(jax.random.fold_in(jax.random.fold_in(stream_key, 6), position), (shards_of,), jnp.float32, low / len(pieces), top_value / len(pieces))
        return jnp.repeat(jnp.exp(steps), shape[position] // shards_of).reshape((-1,) + (1,) * (len(shape) - position - 1))

    factor_of = one(*pieces[0])
    for cut in pieces[1:]:
        factor_of = factor_of * one(*cut)
    return factor_of


def normal_values(own_key, dims, deviation, bound, pieces=(), kind=jnp.bfloat16):
    drawn = deviation * jax.random.normal(own_key, dims, jnp.float32)
    if pieces:
        drawn = drawn * shard_levels(own_key, dims, pieces, -0.22, 0.18)
    return jnp.clip(drawn, -bound, bound).astype(kind)


def setup_inputs(seed: int = 0) -> dict:
    arg_keys = jax.random.split(jax.random.key(seed), 4)
    return {
        "pair_coeffs": normal_values(arg_keys[0], (NAUX, PAIRS), PAIRS ** -0.5, 0.0625, ((0, 4), (1, 8)), jnp.float32),
        "pair_gaps": jnp.clip(jnp.exp(math.log(20.0) - 4.6051702 * jax.random.uniform(arg_keys[1], (PAIRS,), jnp.float32) ** shard_levels(arg_keys[1], (PAIRS,), ((0, 8),), -0.2, 0.2)), 0.2, 20.0),
        "trial_vectors": normal_values(arg_keys[2], (NAUX, K), NAUX ** -0.5, 0.03125, ((0, 4),), jnp.float32),
    }


def project(pair_coeffs, vectors):
    return lax.dot_general(pair_coeffs.astype(jnp.float32), vectors.astype(jnp.float32), (((0,), (0,)), ((), ())), precision=lax.Precision.HIGHEST, preferred_element_type=jnp.float32)

def reference(pair_coeffs, pair_gaps, trial_vectors):
    highest = lax.Precision.HIGHEST
    weights = 4.0 * pair_gaps / (pair_gaps * pair_gaps + 1.0)
    vectors = trial_vectors
    for step in range(ITERS):
        projected = project(pair_coeffs, vectors)
        scaled = weights[:, None] * projected
        applied = jnp.dot(pair_coeffs.astype(jnp.float32), scaled.astype(jnp.float32), precision=highest, preferred_element_type=jnp.float32)
        correlation = jnp.dot(applied.T.astype(jnp.float32), applied.astype(jnp.float32), precision=highest, preferred_element_type=jnp.float32)
        factor = jnp.linalg.cholesky(correlation)
        vectors = jax.scipy.linalg.solve_triangular(factor, applied.T, lower=True).T
    final_proj = project(pair_coeffs, vectors)
    rayleigh = jnp.dot(final_proj.T.astype(jnp.float32), (weights[:, None] * final_proj).astype(jnp.float32), precision=highest, preferred_element_type=jnp.float32)
    return (vectors, rayleigh)
```

```python
import functools

import jax
import jax.numpy as jnp
from jax import lax
from jax.experimental import pallas as pl
from jax.experimental.pallas import tpu as pltpu
from jax.sharding import PartitionSpec as P

ITERS = 2
MESH = pl.DeviceIdType.MESH
F32 = jnp.float32
BF16 = jnp.bfloat16
HIGHEST = lax.Precision.HIGHEST


def split(x):
    hi = x.astype(BF16)
    return hi, (x - hi.astype(F32)).astype(BF16)


def reduce_kernel(axis, n, x_ref, o_ref, got, rs_send, rs_recv, ag_send, ag_recv):
    me = lax.axis_index(axis)
    rows = x_ref.shape[0] // n

    def block(i):
        return pl.ds(pl.multiple_of(i * rows, 8), rows)

    barrier = pltpu.get_barrier_semaphore()
    for d in range(1, n):
        pl.semaphore_signal(barrier, inc=1, device_id={axis: lax.rem(me + d, n)}, device_id_type=MESH)
    pl.semaphore_wait(barrier, n - 1)
    scatter = []
    for d in range(1, n):
        to = lax.rem(me + d, n)
        copy = pltpu.make_async_remote_copy(
            x_ref.at[block(to)], got.at[d - 1], rs_send.at[d - 1], rs_recv.at[d - 1],
            device_id={axis: to}, device_id_type=MESH)
        copy.start()
        scatter.append(copy)
    total = x_ref[block(me), :]
    for d in range(1, n):
        scatter[d - 1].wait_recv()
        total = total + got[d - 1]
    o_ref[block(me), :] = total
    gather = []
    for d in range(1, n):
        copy = pltpu.make_async_remote_copy(
            o_ref.at[block(me)], o_ref.at[block(me)], ag_send.at[d - 1], ag_recv.at[d - 1],
            device_id={axis: lax.rem(me + d, n)}, device_id_type=MESH)
        copy.start()
        gather.append(copy)
    for d in range(1, n):
        frm = lax.rem(me + n - d, n)
        pltpu.make_async_remote_copy(
            o_ref.at[block(frm)], o_ref.at[block(frm)], ag_send.at[d - 1], ag_recv.at[d - 1],
            device_id={axis: lax.rem(me + d, n)}, device_id_type=MESH).wait_recv()
    for d in range(1, n):
        scatter[d - 1].wait_send()
        gather[d - 1].wait_send()


def all_reduce(x, axis, n, collective_id):
    if n == 1:
        return x
    rows, cols = x.shape
    return pl.pallas_call(
        functools.partial(reduce_kernel, axis, n),
        out_shape=jax.ShapeDtypeStruct(x.shape, F32),
        in_specs=[pl.BlockSpec(memory_space=pltpu.VMEM)],
        out_specs=pl.BlockSpec(memory_space=pltpu.VMEM),
        scratch_shapes=[pltpu.VMEM((n - 1, rows // n, cols), F32)] + [pltpu.SemaphoreType.DMA((n - 1,))] * 4,
        compiler_params=pltpu.CompilerParams(collective_id=collective_id, has_side_effects=True),
        name="reduce_" + axis,
    )(x)


def apply_kernel(n, rows, b_ref, *refs):
    if rows % 8:
        tail_ref, *refs = refs
    else:
        tail_ref = None
    (s_ref, a_ref, y_ref, c_ref, bbuf, bhi, blo, s2, own, give, pair, came, cat, b_sem,
     pair_send, pair_recv, rs_send, rs_recv, ag_send, ag_recv, fwd_send, fwd_recv) = refs
    h = n // 2
    me = lax.axis_index("rows")
    z, c = me // 2, lax.rem(me, 2)
    at = z + c * (h - 1 - 2 * z)
    step_to = 1 - 2 * c
    steps, blk, k = own.shape
    pairs = s_ref.shape[0]
    last = rows - (steps - 1) * 2 * blk
    last8 = (last + 7) // 8 * 8
    partner = {"rows": z * 2 + 1 - c}
    following = {"rows": (z + step_to) * 2 + c}
    previous = {"rows": (z - step_to) * 2 + c}
    first, end = at == 0, at == h - 1
    delay = 1 + 5 * at
    back = 4 * (h - 1 - at)
    across = 2 * (h - 1)

    def remote(src, dst, send, recv, to):
        return pltpu.make_async_remote_copy(src, dst, send, recv, device_id=to, device_id_type=MESH)

    def over(i):
        return remote(give.at[i], pair.at[i], pair_send.at[i], pair_recv.at[i], partner)

    def onward(i):
        return remote(own.at[i], came.at[i], rs_send.at[i], rs_recv.at[i], following)

    def backward(i):
        return remote(a_ref.at[2 * i + c], a_ref.at[2 * i + c], ag_send.at[i], ag_recv.at[i], previous)

    def share(i, j):
        return remote(a_ref.at[j], a_ref.at[j], fwd_send.at[i], fwd_recv.at[i], partner)

    def full(i):
        return pltpu.make_async_copy(b_ref.at[pl.ds(pl.multiple_of(i * 2 * blk, 2 * blk), 2 * blk)],
                                     bbuf.at[lax.rem(i, 2)], b_sem.at[lax.rem(i, 2)])

    def short():
        src = tail_ref if rows % 8 else b_ref.at[pl.ds((steps - 1) * 2 * blk, last8)]
        slot = (steps - 1) % 2
        return pltpu.make_async_copy(src, bbuf.at[slot, pl.ds(0, last8)], b_sem.at[slot])

    def start(i):
        @pl.when(i < steps - 1)
        def _():
            full(i).start()

        @pl.when(i == steps - 1)
        def _():
            short().start()

    start(jnp.int32(0))
    start(jnp.int32(1))
    hi, lo = split(s_ref[...])
    s2[:, :k] = hi
    s2[:, k:] = lo
    y_ref[...] = jnp.zeros_like(y_ref)
    c_ref[...] = jnp.zeros_like(c_ref)

    barrier = pltpu.get_barrier_semaphore()
    pl.semaphore_signal(barrier, inc=1, device_id=partner, device_id_type=MESH)

    @pl.when(jnp.logical_not(end))
    def _():
        pl.semaphore_signal(barrier, inc=1, device_id=following, device_id_type=MESH)

    @pl.when(jnp.logical_not(first))
    def _():
        pl.semaphore_signal(barrier, inc=1, device_id=previous, device_id_type=MESH)

    pl.semaphore_wait(barrier, 1 + jnp.minimum(at, 1) + jnp.minimum(h - 1 - at, 1))

    def product(i, half):
        where = pl.ds(pl.multiple_of(half * blk, blk), blk)
        keep = pl.ds(pl.multiple_of(i * 2 * blk + half * blk, blk), blk)
        high, low = split(bbuf[lax.rem(i, 2), where, :])
        bhi[keep, :] = high
        blo[keep, :] = low
        wide = jnp.dot(high, s2[...], preferred_element_type=F32)
        thin = jnp.dot(low, s2[:, :k], preferred_element_type=F32)
        return wide[:, :k] + (wide[:, k:] + thin)

    def multiply(i):
        @pl.when(i < steps - 1)
        def _():
            full(i).wait()

        @pl.when(i == steps - 1)
        def _():
            short().wait()
            if last8 < 2 * blk:
                bbuf[(steps - 1) % 2, pl.ds(last8, 2 * blk - last8), :] = jnp.zeros((2 * blk - last8, pairs), F32)

        give[i] = product(i, 1 - c)
        over(i).start()
        own[i] = product(i, c)
        start(i + 2)

    def reduce(i):
        over(i).wait_recv()
        own[i] = own[i] + pair[i]

        @pl.when(jnp.logical_not(first))
        def _():
            onward(i).wait_recv()
            own[i] = own[i] + came[i]

        @pl.when(jnp.logical_not(end))
        def _():
            onward(i).start()

        @pl.when(end)
        def _():
            a_ref[2 * i + c] = own[i]
            backward(i).start()
            share(i, 2 * i + c).start()

    def project(j):
        a = a_ref[j]
        turned = a.T
        c_ref[...] += lax.dot_general(turned, a, (((1,), (0,)), ((), ())), precision=HIGHEST,
                                      preferred_element_type=F32)
        high, low = split(turned)
        cat[:k, :] = high
        cat[k:, :] = low
        keep = pl.ds(pl.multiple_of(j * blk, blk), blk)
        for t in range(pairs // 256):
            cols = pl.ds(t * 256, 256)
            wide = jnp.dot(cat[...], bhi[keep, cols], preferred_element_type=F32)
            thin = jnp.dot(cat[:k, :], blo[keep, cols], preferred_element_type=F32)
            y_ref[:, cols] += wide[:k] + (wide[k:] + thin)

    def body(t, carry):
        @pl.when(t < steps)
        def _():
            multiply(t)

        i = t - delay

        @pl.when(jnp.logical_and(i >= 0, i < steps))
        def _():
            reduce(i)

        i = t - delay - back

        @pl.when(jnp.logical_and(i >= 0, i < steps))
        def _():
            @pl.when(jnp.logical_not(end))
            def _():
                backward(i).wait_recv()
                share(i, 2 * i + c).start()

                @pl.when(jnp.logical_not(first))
                def _():
                    backward(i).start()

            project(2 * i + c)

        i = t - delay - across

        @pl.when(jnp.logical_and(i >= 0, i < steps))
        def _():
            share(i, 2 * i + 1 - c).wait_recv()
            project(2 * i + 1 - c)

        return carry

    total = steps + 1 + 5 * (h - 1) + max(2 * (h - 1), 4 * (h - 1) - 5 * (h - 1))
    lax.fori_loop(0, total, body, 0)

    def drain(i, carry):
        over(i).wait_send()
        share(i, 2 * i + c).wait_send()

        @pl.when(jnp.logical_not(end))
        def _():
            onward(i).wait_send()

        @pl.when(jnp.logical_not(first))
        def _():
            backward(i).wait_send()

        return carry

    lax.fori_loop(0, steps, drain, 0)


def apply(b, s, n):
    rows = b.shape[0]
    pairs, k = s.shape
    blk = 256
    steps = (rows + 2 * blk - 1) // (2 * blk)
    dma = pltpu.SemaphoreType.DMA
    vmem = pl.BlockSpec(memory_space=pltpu.VMEM)
    anywhere = pl.BlockSpec(memory_space=pl.ANY)
    operands = [b]
    if rows % 8:
        operands.append(jnp.pad(b[(steps - 1) * 2 * blk:], ((0, -rows % 8), (0, 0))))
    return pl.pallas_call(
        functools.partial(apply_kernel, n, rows),
        out_shape=(jax.ShapeDtypeStruct((2 * steps, blk, k), F32), jax.ShapeDtypeStruct((k, pairs), F32),
                   jax.ShapeDtypeStruct((k, k), F32)),
        in_specs=[anywhere] * len(operands) + [vmem],
        out_specs=(vmem, vmem, vmem),
        scratch_shapes=[
            pltpu.VMEM((2, 2 * blk, pairs), F32),
            pltpu.VMEM((2 * steps * blk, pairs), BF16),
            pltpu.VMEM((2 * steps * blk, pairs), BF16),
            pltpu.VMEM((pairs, 2 * k), BF16),
            pltpu.VMEM((steps, blk, k), F32),
            pltpu.VMEM((steps, blk, k), F32),
            pltpu.VMEM((steps, blk, k), F32),
            pltpu.VMEM((steps, blk, k), F32),
            pltpu.VMEM((2 * k, blk), BF16),
            dma((2,)),
        ] + [dma((steps,))] * 8,
        compiler_params=pltpu.CompilerParams(collective_id=0, has_side_effects=True,
                                             vmem_limit_bytes=63 * 1024 * 1024),
        name="apply",
    )(*operands, s)


def solution(mesh):
    n = mesh.shape["rows"]
    aux = mesh.shape["aux"]

    def shards(b, gaps, trial):
        rows, k = trial.shape
        weights = (4.0 * gaps / (gaps * gaps + 1.0))[None, :]
        yt = lax.dot_general(trial, b, (((0,), (0,)), ((), ())), precision=lax.Precision.HIGH,
                             preferred_element_type=F32)
        pt = all_reduce(yt, "aux", aux, 1)
        for step in range(ITERS):
            a, yt, gram = apply(b, (pt * weights).T, n)
            both = all_reduce(jnp.concatenate([yt, gram], axis=1), "aux", aux, 2)
            factor = jnp.linalg.cholesky(both[:, -k:])
            inverse = jax.scipy.linalg.solve_triangular(factor, jnp.eye(k, dtype=F32), lower=True)
            pt = jnp.dot(inverse, both[:, :-k], precision=HIGHEST, preferred_element_type=F32)
        v = lax.dot_general(a, inverse, (((2,), (1,)), ((), ())), precision=lax.Precision.HIGH,
                            preferred_element_type=F32)
        vectors = v.reshape(-1, k)[:rows]
        part = lax.dot_general(pt, pt * weights, (((1,), (1,)), ((), ())), precision=HIGHEST,
                               preferred_element_type=F32)
        return vectors, all_reduce(part, "rows", n, 3)

    in_specs = (P("aux", "rows"), P("rows"), P("aux", None))
    return jax.shard_map(shards, mesh=mesh, in_specs=in_specs, out_specs=(P("aux", None), P()), check_vma=False)
```

```python
import functools

import jax
import jax.numpy as jnp
from jax import lax
from jax.experimental import pallas as pl
from jax.experimental.pallas import tpu as pltpu
from jax.sharding import PartitionSpec as P

ITERS = 2
MESH = pl.DeviceIdType.MESH
F32 = jnp.float32
BF16 = jnp.bfloat16
HIGHEST = lax.Precision.HIGHEST


def split(x):
    hi = x.astype(BF16)
    return hi, (x - hi.astype(F32)).astype(BF16)


def kernel(n, m, rows, iters, b_ref, *refs):
    if rows % 8:
        tail_ref, *refs = refs
    else:
        tail_ref = None
    (t_ref, w_ref, v_ref, r_ref, a_ref, bbuf, bhi, blo, s2, own, give, pair, came, cat, y_ref, c_ref,
     whole, got, grams, left, inv, part, gotr,
     b_sem, t_sem, v_sem, pair_send, pair_recv, line_send, line_recv, back_send, back_recv, fwd_send, fwd_recv,
     rs_send, rs_recv, ag_send, ag_recv, g_send, g_recv, r_send, r_recv, q_send, q_recv) = refs
    h = n // 2
    me, mine = lax.axis_index("rows"), lax.axis_index("aux")
    z, c = me // 2, lax.rem(me, 2)
    at = z + c * (h - 1 - 2 * z)
    step_to = 1 - 2 * c
    steps, blk, k = own.shape
    pairs = bhi.shape[1]
    width = pairs // m
    last = rows - (steps - 1) * 2 * blk
    last8 = (last + 7) // 8 * 8
    rows8 = (rows + 7) // 8 * 8
    partner = {"rows": z * 2 + 1 - c}
    following = {"rows": (z + step_to) * 2 + c}
    previous = {"rows": (z - step_to) * 2 + c}
    first, end = at == 0, at == h - 1
    lag = 6
    delay = 1 + 4 * at
    back = 6 * (h - 1 - at) + lag
    across = 3 * (h - 1) + lag

    def remote(src, dst, send, recv, to):
        return pltpu.make_async_remote_copy(src, dst, send, recv, device_id=to, device_id_type=MESH)

    def chunk(j):
        return pl.ds(pl.multiple_of(j * blk, blk), blk)

    def column(i):
        return pl.ds(pl.multiple_of(i * width, 128), width)

    def peer(d):
        return {"aux": lax.rem(mine + d, m)}

    barrier = pltpu.get_barrier_semaphore()
    for d in range(1, n):
        pl.semaphore_signal(barrier, inc=1, device_id={"rows": lax.rem(me + d, n)}, device_id_type=MESH)
    for d in range(1, m):
        pl.semaphore_signal(barrier, inc=1, device_id=peer(d), device_id_type=MESH)

    def full(i):
        return pltpu.make_async_copy(b_ref.at[pl.ds(pl.multiple_of(i * 2 * blk, 2 * blk), 2 * blk)],
                                     bbuf.at[lax.rem(i, 2)], b_sem.at[lax.rem(i, 2)])

    def short():
        src = tail_ref if rows % 8 else b_ref.at[pl.ds((steps - 1) * 2 * blk, last8)]
        slot = (steps - 1) % 2
        return pltpu.make_async_copy(src, bbuf.at[slot, pl.ds(0, last8)], b_sem.at[slot])

    def start(i):
        @pl.when(i < steps - 1)
        def _():
            full(i).start()

        @pl.when(i == steps - 1)
        def _():
            short().start()

    trial = pltpu.make_async_copy(t_ref, a_ref.at[pl.ds(0, rows8)], t_sem.at[0])
    trial.start()
    start(jnp.int32(0))
    start(jnp.int32(1))
    if rows8 < 2 * steps * blk:
        a_ref[pl.ds(rows8, 2 * steps * blk - rows8), :] = jnp.zeros((2 * steps * blk - rows8, k), F32)
    y_ref[...] = jnp.zeros_like(y_ref)
    trial.wait()

    def project(j, with_gram):
        a = a_ref[chunk(j), :]
        turned = a.T
        if with_gram:
            c_ref[...] += lax.dot_general(turned, a, (((1,), (0,)), ((), ())), precision=HIGHEST,
                                          preferred_element_type=F32)
        high, low = split(turned)
        cat[:k, :] = high
        cat[k:, :] = low
        for t in range(pairs // 256):
            cols = pl.ds(t * 256, 256)
            wide = jnp.dot(cat[...], bhi[chunk(j), cols], preferred_element_type=F32)
            thin = jnp.dot(cat[:k, :], blo[chunk(j), cols], preferred_element_type=F32)
            y_ref[:, cols] += wide[:k] + (wide[k:] + thin)

    def load(i, carry):
        @pl.when(i < steps - 1)
        def _():
            full(i).wait()

        @pl.when(i == steps - 1)
        def _():
            short().wait()
            if last8 < 2 * blk:
                bbuf[(steps - 1) % 2, pl.ds(last8, 2 * blk - last8), :] = jnp.zeros((2 * blk - last8, pairs), F32)

        for half in range(2):
            high, low = split(bbuf[lax.rem(i, 2), pl.ds(half * blk, blk), :])
            bhi[chunk(2 * i + half), :] = high
            blo[chunk(2 * i + half), :] = low
        start(i + 2)
        project(2 * i, False)
        project(2 * i + 1, False)
        return carry

    lax.fori_loop(0, steps, load, 0)
    pl.semaphore_wait(barrier, n - 1 + m - 1)

    group = 4

    def eliminate(g, carry):
        j = g * group
        a, x = left[...], inv[...]
        u = [left[pl.ds(j + q, 1), :] for q in range(group)]
        v = [inv[pl.ds(j + q, 1), :] for q in range(group)]
        col = [a[:, q:q + 1] for q in range(group)]
        small = [[u[q][:, p:p + 1] for p in range(group)] for q in range(group)]
        over, low = [], []
        for p in range(group):
            over.append(1.0 / small[p][p])
            for q in range(p + 1, group):
                f = small[q][p] * over[p]
                u[q] = u[q] - f * u[p]
                v[q] = v[q] - f * v[p]
                for r in range(p + 1, group):
                    small[q][r] = small[q][r] - f * small[p][r]
        below = lax.broadcasted_iota(jnp.int32, (k, 1), 0) >= j + group
        for q in range(group):
            top = col[q]
            for p in range(q):
                top = top - low[p] * small[p][q]
            low.append(jnp.where(below, top * over[q], 0.0))
        for q in range(group):
            a = a - low[q] * u[q]
            x = x - low[q] * v[q]
        left[...] = pltpu.roll(a, k - group, 1)
        inv[...] = x
        for q in range(group):
            inv[pl.ds(j + q, 1), :] = v[q] / jnp.sqrt(small[q][q])
        return carry

    def between(e):
        def gram(d, whose):
            return remote(c_ref, grams.at[whose], g_send.at[e, d - 1], g_recv.at[e, d - 1], peer(d))

        def scatter(d):
            return remote(y_ref.at[:, column(lax.rem(mine + d, m))], got.at[d - 1],
                          rs_send.at[e, d - 1], rs_recv.at[e, d - 1], peer(d))

        def gather(d, whose):
            return remote(whole.at[:, column(whose)], whole.at[:, column(whose)],
                          ag_send.at[e, d - 1], ag_recv.at[e, d - 1], peer(d))

        if e:
            for d in range(1, m):
                gram(d, mine).start()
        for d in range(1, m):
            scatter(d).start()

        def sums():
            total = y_ref[:, column(mine)]
            for d in range(1, m):
                scatter(d).wait_recv()
                total = total + got[d - 1]
            whole[:, column(mine)] = total
            for d in range(1, m):
                gather(d, mine).start()

        if e:
            grams[mine] = c_ref[...]
            for d in range(1, m):
                gram(d, lax.rem(mine + m - d, m)).wait_recv()
            total = grams[0]
            for i in range(1, m):
                total = total + grams[i]
            left[...] = total
            inv[...] = (lax.broadcasted_iota(jnp.int32, (k, k), 0)
                        == lax.broadcasted_iota(jnp.int32, (k, k), 1)).astype(F32)
            lax.fori_loop(0, k // group // 2, eliminate, 0)
            sums()
            lax.fori_loop(k // group // 2, k // group, eliminate, 0)
        else:
            sums()
        for d in range(1, m):
            gather(d, lax.rem(mine + m - d, m)).wait_recv()
        if e == iters:
            part[...] = jnp.zeros_like(part)
        for t in range(pairs // 256):
            cols = pl.ds(t * 256, 256)
            pt = whole[:, cols]
            if e:
                pt = jnp.dot(inv[...], pt, precision=HIGHEST, preferred_element_type=F32)
            scaled = pt * w_ref[:, cols]
            if e == iters:
                part[...] += lax.dot_general(pt, scaled, (((1,), (1,)), ((), ())), precision=HIGHEST,
                                             preferred_element_type=F32)
            else:
                high, low = split(scaled.T)
                s2[cols, :k] = high
                s2[cols, k:] = low
        for d in range(1, m):
            if e:
                gram(d, mine).wait_send()
            scatter(d).wait_send()
            gather(d, mine).wait_send()

    def line(e):
        def over(i):
            return remote(give.at[i], pair.at[i], pair_send.at[e, i], pair_recv.at[e, i], partner)

        def onward(i):
            return remote(own.at[i], came.at[i], line_send.at[e, i], line_recv.at[e, i], following)

        def backward(i):
            return remote(a_ref.at[chunk(2 * i + c)], a_ref.at[chunk(2 * i + c)],
                          back_send.at[e, i], back_recv.at[e, i], previous)

        def share(i, j):
            return remote(a_ref.at[chunk(j)], a_ref.at[chunk(j)], fwd_send.at[e, i], fwd_recv.at[e, i], partner)

        def product(j):
            wide = jnp.dot(bhi[chunk(j), :], s2[...], preferred_element_type=F32)
            thin = jnp.dot(blo[chunk(j), :], s2[:, :k], preferred_element_type=F32)
            return wide[:, :k] + (wide[:, k:] + thin)

        def multiply(i):
            give[i] = product(2 * i + 1 - c)
            over(i).start()
            own[i] = product(2 * i + c)

        def reduce(i):
            over(i).wait_recv()
            own[i] = own[i] + pair[i]

            @pl.when(jnp.logical_not(first))
            def _():
                onward(i).wait_recv()
                own[i] = own[i] + came[i]

            @pl.when(jnp.logical_not(end))
            def _():
                onward(i).start()

            @pl.when(end)
            def _():
                a_ref[chunk(2 * i + c), :] = own[i]

        y_ref[...] = jnp.zeros_like(y_ref)
        c_ref[...] = jnp.zeros_like(c_ref)

        def step(t, carry):
            @pl.when(t < steps)
            def _():
                multiply(t)

            i = t - delay

            @pl.when(jnp.logical_and(i >= 0, i < steps))
            def _():
                reduce(i)

            i = t - delay - back

            @pl.when(jnp.logical_and(i >= 0, i < steps))
            def _():
                @pl.when(jnp.logical_not(end))
                def _():
                    backward(i).wait_recv()

                @pl.when(jnp.logical_not(first))
                def _():
                    backward(i).start()

                share(i, 2 * i + c).start()
                project(2 * i + c, True)

            i = t - delay - across

            @pl.when(jnp.logical_and(i >= 0, i < steps))
            def _():
                share(i, 2 * i + 1 - c).wait_recv()
                project(2 * i + 1 - c, True)

            return carry

        lax.fori_loop(0, steps + 1 + 4 * (h - 1) + 6 * (h - 1) + lag, step, 0)

        def drain(i, carry):
            over(i).wait_send()
            share(i, 2 * i + c).wait_send()

            @pl.when(jnp.logical_not(end))
            def _():
                onward(i).wait_send()

            @pl.when(jnp.logical_not(first))
            def _():
                backward(i).wait_send()

            return carry

        lax.fori_loop(0, steps, drain, 0)

    between(0)
    for e in range(iters):
        line(e)
        between(e + 1)

    slab = k // n

    def strip(i):
        return pl.ds(pl.multiple_of(i * slab, 8), slab)

    def scatter(d):
        to = lax.rem(me + d, n)
        return remote(part.at[strip(to)], gotr.at[d - 1], r_send.at[d - 1], r_recv.at[d - 1], {"rows": to})

    def gather(d, whose):
        return remote(r_ref.at[strip(whose)], r_ref.at[strip(whose)], q_send.at[d - 1], q_recv.at[d - 1],
                      {"rows": lax.rem(me + d, n)})

    for d in range(1, n):
        scatter(d).start()

    def rotate(j, carry):
        a_ref[chunk(j), :] = lax.dot_general(a_ref[chunk(j), :], inv[...], (((1,), (1,)), ((), ())),
                                             precision=HIGHEST, preferred_element_type=F32)
        return carry

    lax.fori_loop(0, steps, rotate, 0)
    total = part[strip(me), :]
    for d in range(1, n):
        scatter(d).wait_recv()
        total = total + gotr[d - 1]
    r_ref[strip(me), :] = total
    for d in range(1, n):
        gather(d, me).start()
    lax.fori_loop(steps, 2 * steps, rotate, 0)
    done = pltpu.make_async_copy(a_ref.at[pl.ds(0, rows8)], v_ref, v_sem.at[0])
    done.start()
    for d in range(1, n):
        gather(d, lax.rem(me + n - d, n)).wait_recv()
    for d in range(1, n):
        scatter(d).wait_send()
        gather(d, me).wait_send()
    done.wait()


def solution(mesh):
    n = mesh.shape["rows"]
    m = mesh.shape["aux"]

    def shards(b, gaps, trial):
        rows, k = trial.shape
        pairs = b.shape[1]
        blk = 256
        steps = (rows + 2 * blk - 1) // (2 * blk)
        rows8 = (rows + 7) // 8 * 8
        weights = (4.0 * gaps / (gaps * gaps + 1.0))[None, :]
        dma = pltpu.SemaphoreType.DMA
        vmem = pl.BlockSpec(memory_space=pltpu.VMEM)
        anywhere = pl.BlockSpec(memory_space=pl.ANY)
        operands = [b]
        if rows % 8:
            operands.append(jnp.pad(b[(steps - 1) * 2 * blk:], ((0, -rows % 8), (0, 0))))
            trial = jnp.pad(trial, ((0, -rows % 8), (0, 0)))
        operands.append(trial)
        vectors, rayleigh = pl.pallas_call(
            functools.partial(kernel, n, m, rows, ITERS),
            out_shape=(jax.ShapeDtypeStruct((rows8, k), F32), jax.ShapeDtypeStruct((k, k), F32)),
            in_specs=[anywhere] * len(operands) + [vmem],
            out_specs=(anywhere, vmem),
            scratch_shapes=[
                pltpu.VMEM((2 * steps * blk, k), F32),
                pltpu.VMEM((2, 2 * blk, pairs), F32),
                pltpu.VMEM((2 * steps * blk, pairs), BF16),
                pltpu.VMEM((2 * steps * blk, pairs), BF16),
                pltpu.VMEM((pairs, 2 * k), BF16),
                pltpu.VMEM((steps, blk, k), F32),
                pltpu.VMEM((steps, blk, k), F32),
                pltpu.VMEM((steps, blk, k), F32),
                pltpu.VMEM((steps, blk, k), F32),
                pltpu.VMEM((2 * k, blk), BF16),
                pltpu.VMEM((k, pairs), F32),
                pltpu.VMEM((k, k), F32),
                pltpu.VMEM((k, pairs), F32),
                pltpu.VMEM((m - 1, k, pairs // m), F32),
                pltpu.VMEM((m, k, k), F32),
                pltpu.VMEM((k, k), F32),
                pltpu.VMEM((k, k), F32),
                pltpu.VMEM((k, k), F32),
                pltpu.VMEM((n - 1, k // n, k), F32),
                dma((2,)), dma((1,)), dma((1,)),
            ] + [dma((ITERS, steps))] * 8 + [dma((ITERS + 1, m - 1))] * 6 + [dma((n - 1,))] * 4,
            compiler_params=pltpu.CompilerParams(collective_id=0, has_side_effects=True,
                                                 vmem_limit_bytes=63 * 1024 * 1024),
            name="subspace",
        )(*operands, weights)
        return vectors[:rows], rayleigh

    in_specs = (P("aux", "rows"), P("rows"), P("aux", None))
    return jax.shard_map(shards, mesh=mesh, in_specs=in_specs, out_specs=(P("aux", None), P()), check_vma=False)
```

```python
import functools

import jax
import jax.numpy as jnp
from jax import lax
from jax.experimental import pallas as pl
from jax.experimental.pallas import tpu as pltpu
from jax.sharding import PartitionSpec as P

ITERS = 2
MESH = pl.DeviceIdType.MESH
F32 = jnp.float32
BF16 = jnp.bfloat16
HIGHEST = lax.Precision.HIGHEST


def split(x):
    hi = x.astype(BF16)
    return hi, (x - hi.astype(F32)).astype(BF16)


def kernel(n, m, rows, iters, b_ref, *refs):
    if rows % 8:
        tail_ref, *refs = refs
    else:
        tail_ref = None
    (t_ref, gap_ref, v_ref, i_ref, r_ref, a_ref, bbuf, bhi, blo, s2, own, give, pair, came, cat, y_ref, c_ref,
     whole, got, grams, left, inv, part, gotr, w_ref,
     b_sem, t_sem, v_sem, pair_send, pair_recv, line_send, line_recv, back_send, back_recv, fwd_send, fwd_recv,
     rs_send, rs_recv, ag_send, ag_recv, g_send, g_recv, r_send, r_recv, q_send, q_recv) = refs
    h = n // 2
    me, mine = lax.axis_index("rows"), lax.axis_index("aux")
    z, c = me // 2, lax.rem(me, 2)
    at = z + c * (h - 1 - 2 * z)
    step_to = 1 - 2 * c
    steps, blk, k = own.shape
    pairs = bhi.shape[1]
    width = pairs // m
    last = rows - (steps - 1) * 2 * blk
    last8 = (last + 7) // 8 * 8
    rows8 = (rows + 7) // 8 * 8
    partner = {"rows": z * 2 + 1 - c}
    following = {"rows": (z + step_to) * 2 + c}
    previous = {"rows": (z - step_to) * 2 + c}
    first, end = at == 0, at == h - 1
    lag, ahead, behind = 6, 4, 6
    delay = 1 + ahead * at
    back = behind * (h - 1 - at) + lag
    across = behind // 2 * (h - 1) + lag

    def remote(src, dst, send, recv, to):
        return pltpu.make_async_remote_copy(src, dst, send, recv, device_id=to, device_id_type=MESH)

    def chunk(j):
        return pl.ds(pl.multiple_of(j * blk, blk), blk)

    def column(i):
        return pl.ds(pl.multiple_of(i * width, 128), width)

    def peer(d):
        return {"aux": lax.rem(mine + d, m)}

    barrier = pltpu.get_barrier_semaphore()
    for d in range(1, n):
        pl.semaphore_signal(barrier, inc=1, device_id={"rows": lax.rem(me + d, n)}, device_id_type=MESH)
    for d in range(1, m):
        pl.semaphore_signal(barrier, inc=1, device_id=peer(d), device_id_type=MESH)

    def full(i):
        return pltpu.make_async_copy(b_ref.at[pl.ds(pl.multiple_of(i * 2 * blk, 2 * blk), 2 * blk)],
                                     bbuf.at[lax.rem(i, 2)], b_sem.at[lax.rem(i, 2)])

    def short():
        src = tail_ref if rows % 8 else b_ref.at[pl.ds((steps - 1) * 2 * blk, last8)]
        slot = (steps - 1) % 2
        return pltpu.make_async_copy(src, bbuf.at[slot, pl.ds(0, last8)], b_sem.at[slot])

    def start(i):
        @pl.when(i < steps - 1)
        def _():
            full(i).start()

        @pl.when(i == steps - 1)
        def _():
            short().start()

    trial = pltpu.make_async_copy(t_ref, a_ref.at[pl.ds(0, rows8)], t_sem.at[0])
    trial.start()
    start(jnp.int32(0))
    start(jnp.int32(1))
    if rows8 < 2 * steps * blk:
        a_ref[pl.ds(rows8, 2 * steps * blk - rows8), :] = jnp.zeros((2 * steps * blk - rows8, k), F32)
    y_ref[...] = jnp.zeros_like(y_ref)
    gap = gap_ref[...]
    w_ref[...] = 4.0 * gap / (gap * gap + 1.0)
    trial.wait()

    def project(at_row, size, with_gram):
        where = pl.ds(pl.multiple_of(at_row, blk), size)
        a = a_ref[where, :]
        turned = a.T
        if with_gram:
            c_ref[...] += lax.dot_general(turned, a, (((1,), (0,)), ((), ())), precision=HIGHEST,
                                          preferred_element_type=F32)
        high, low = split(turned)
        cat[:k, :size] = high
        cat[k:, :size] = low
        for t in range(pairs // 256):
            cols = pl.ds(t * 256, 256)
            wide = jnp.dot(cat[:, :size], bhi[where, cols], preferred_element_type=F32)
            thin = jnp.dot(cat[:k, :size], blo[where, cols], preferred_element_type=F32)
            y_ref[:, cols] += wide[:k] + (wide[k:] + thin)

    def load(i, carry):
        @pl.when(i < steps - 1)
        def _():
            full(i).wait()

        @pl.when(i == steps - 1)
        def _():
            short().wait()
            if last8 < 2 * blk:
                bbuf[(steps - 1) % 2, pl.ds(last8, 2 * blk - last8), :] = jnp.zeros((2 * blk - last8, pairs), F32)

        for half in range(2):
            high, low = split(bbuf[lax.rem(i, 2), pl.ds(half * blk, blk), :])
            bhi[chunk(2 * i + half), :] = high
            blo[chunk(2 * i + half), :] = low
        start(i + 2)
        project(2 * i * blk, 2 * blk, False)
        return carry

    lax.fori_loop(0, steps, load, 0)
    pl.semaphore_wait(barrier, n - 1 + m - 1)

    group = 8

    def eliminate(tiles):
        def clear(g, carry):
            j = g * group
            u = [jnp.broadcast_to(left[pl.ds(j + q, 1), :], (8, k)) for q in range(group)]
            v = [jnp.broadcast_to(inv[pl.ds(j + q, 1), :], (8, k)) for q in range(group)]
            small = [[jnp.broadcast_to(u[q][:, p:p + 1], (8, k)) for p in range(group)] for q in range(group)]
            over = []
            for p in range(group):
                over.append(1.0 / small[p][p])
                for q in range(p + 1, group):
                    f = small[q][p] * over[p]
                    u[q] = u[q] - f * u[p]
                    v[q] = v[q] - f * v[p]
                    for r in range(p + 1, group):
                        small[q][r] = small[q][r] - f * small[p][r]
            kept = [v[q] / jnp.sqrt(small[q][q]) for q in range(group)]
            for p in reversed(range(group)):
                for q in range(p + 1, group):
                    u[p] = u[p] - small[p][q] * u[q]
                    v[p] = v[p] - small[p][q] * v[q]
                u[p] = u[p] * over[p]
                v[p] = v[p] * over[p]
            for t in tiles:
                tile = pl.ds(t * 8, 8)
                a, x = left[tile, :], inv[tile, :]
                below = lax.broadcasted_iota(jnp.int32, (8, k), 0) + t * 8 >= j + group
                for q in range(group):
                    f = jnp.where(below, left[tile, q:q + 1], 0.0)
                    a = a - f * u[q]
                    x = x - f * v[q]
                left[tile, :] = pltpu.roll(a, k - group, 1)
                inv[tile, :] = x
            for q in range(group):
                inv[pl.ds(j + q, 1), :] = kept[q][:1]
            return carry

        return clear

    def between(e):
        def gram(d, whose):
            return remote(c_ref, grams.at[whose], g_send.at[e, d - 1], g_recv.at[e, d - 1], peer(d))

        def scatter(d):
            return remote(y_ref.at[:, column(lax.rem(mine + d, m))], got.at[d - 1],
                          rs_send.at[e, d - 1], rs_recv.at[e, d - 1], peer(d))

        def gather(d, whose):
            return remote(whole.at[:, column(whose)], whole.at[:, column(whose)],
                          ag_send.at[e, d - 1], ag_recv.at[e, d - 1], peer(d))

        if e:
            for d in range(1, m):
                gram(d, mine).start()
        for d in range(1, m):
            scatter(d).start()

        def sums():
            total = y_ref[:, column(mine)]
            for d in range(1, m):
                scatter(d).wait_recv()
                total = total + got[d - 1]
            whole[:, column(mine)] = total
            for d in range(1, m):
                gather(d, mine).start()

        if e:
            grams[mine] = c_ref[...]
            for d in range(1, m):
                gram(d, lax.rem(mine + m - d, m)).wait_recv()
            total = grams[0]
            for i in range(1, m):
                total = total + grams[i]
            left[...] = total
            inv[...] = (lax.broadcasted_iota(jnp.int32, (k, k), 0)
                        == lax.broadcasted_iota(jnp.int32, (k, k), 1)).astype(F32)
            lax.fori_loop(0, k // group // 2, eliminate(range(k // 8)), 0)
            sums()
            lax.fori_loop(k // group // 2, k // group, eliminate(range(k // 16, k // 8)), 0)
        else:
            sums()
        for d in range(1, m):
            gather(d, lax.rem(mine + m - d, m)).wait_recv()
        if e == iters:
            part[...] = jnp.zeros_like(part)
        for t in range(pairs // 256):
            cols = pl.ds(t * 256, 256)
            pt = whole[:, cols]
            if e:
                pt = jnp.dot(inv[...], pt, precision=HIGHEST, preferred_element_type=F32)
            scaled = pt * w_ref[:, cols]
            if e == iters:
                part[...] += lax.dot_general(pt, scaled, (((1,), (1,)), ((), ())), precision=HIGHEST,
                                             preferred_element_type=F32)
            else:
                high, low = split(scaled.T)
                s2[cols, :k] = high
                s2[cols, k:] = low
        for d in range(1, m):
            if e:
                gram(d, mine).wait_send()
            scatter(d).wait_send()
            gather(d, mine).wait_send()

    def line(e):
        def over(i):
            return remote(give.at[i], pair.at[i], pair_send.at[e, i], pair_recv.at[e, i], partner)

        def onward(i):
            return remote(own.at[i], came.at[i], line_send.at[e, i], line_recv.at[e, i], following)

        def backward(i):
            return remote(a_ref.at[chunk(2 * i + c)], a_ref.at[chunk(2 * i + c)],
                          back_send.at[e, i], back_recv.at[e, i], previous)

        def share(i, j):
            return remote(a_ref.at[chunk(j)], a_ref.at[chunk(j)], fwd_send.at[e, i], fwd_recv.at[e, i], partner)

        def product(j):
            wide = jnp.dot(bhi[chunk(j), :], s2[...], preferred_element_type=F32)
            thin = jnp.dot(blo[chunk(j), :], s2[:, :k], preferred_element_type=F32)
            return wide[:, :k] + (wide[:, k:] + thin)

        def multiply(i):
            give[i] = product(2 * i + 1 - c)
            over(i).start()
            own[i] = product(2 * i + c)

        def reduce(i):
            over(i).wait_recv()
            own[i] = own[i] + pair[i]

            @pl.when(jnp.logical_not(first))
            def _():
                onward(i).wait_recv()
                own[i] = own[i] + came[i]

            @pl.when(jnp.logical_not(end))
            def _():
                onward(i).start()

            @pl.when(end)
            def _():
                a_ref[chunk(2 * i + c), :] = own[i]

        y_ref[...] = jnp.zeros_like(y_ref)
        c_ref[...] = jnp.zeros_like(c_ref)

        def step(t, carry):
            @pl.when(t < steps)
            def _():
                multiply(t)

            i = t - delay

            @pl.when(jnp.logical_and(i >= 0, i < steps))
            def _():
                reduce(i)

            i = t - delay - back

            @pl.when(jnp.logical_and(i >= 0, i < steps))
            def _():
                @pl.when(jnp.logical_not(end))
                def _():
                    backward(i).wait_recv()

                @pl.when(jnp.logical_not(first))
                def _():
                    backward(i).start()

                share(i, 2 * i + c).start()
                project((2 * i + c) * blk, blk, True)

            i = t - delay - across

            @pl.when(jnp.logical_and(i >= 0, i < steps))
            def _():
                share(i, 2 * i + 1 - c).wait_recv()
                project((2 * i + 1 - c) * blk, blk, True)

            return carry

        lax.fori_loop(0, steps + 1 + (ahead + behind) * (h - 1) + lag, step, 0)

        def drain(i, carry):
            over(i).wait_send()
            share(i, 2 * i + c).wait_send()

            @pl.when(jnp.logical_not(end))
            def _():
                onward(i).wait_send()

            @pl.when(jnp.logical_not(first))
            def _():
                backward(i).wait_send()

            return carry

        lax.fori_loop(0, steps, drain, 0)

    between(0)
    for e in range(iters):
        line(e)
        if e == iters - 1:
            done = pltpu.make_async_copy(a_ref.at[pl.ds(0, rows8)], v_ref, v_sem.at[0])
            done.start()
        between(e + 1)
    i_ref[...] = inv[...]

    slab = k // n

    def strip(i):
        return pl.ds(pl.multiple_of(i * slab, 8), slab)

    def scatter(d):
        to = lax.rem(me + d, n)
        return remote(part.at[strip(to)], gotr.at[d - 1], r_send.at[d - 1], r_recv.at[d - 1], {"rows": to})

    def gather(d, whose):
        return remote(r_ref.at[strip(whose)], r_ref.at[strip(whose)], q_send.at[d - 1], q_recv.at[d - 1],
                      {"rows": lax.rem(me + d, n)})

    for d in range(1, n):
        scatter(d).start()

    total = part[strip(me), :]
    for d in range(1, n):
        scatter(d).wait_recv()
        total = total + gotr[d - 1]
    r_ref[strip(me), :] = total
    for d in range(1, n):
        gather(d, me).start()
    for d in range(1, n):
        gather(d, lax.rem(me + n - d, n)).wait_recv()
    for d in range(1, n):
        scatter(d).wait_send()
        gather(d, me).wait_send()
    done.wait()


def rotate_kernel(a_ref, i_ref, v_ref):
    def thirds(x):
        high, rest = x.astype(BF16), x - x.astype(BF16).astype(F32)
        return (high,) + split(rest)

    high, mid, low = thirds(a_ref[...])
    ihigh, imid, ilow = thirds(i_ref[...].T)
    k = ihigh.shape[1]
    both = jnp.concatenate([jnp.concatenate([ihigh, imid], axis=1), jnp.concatenate([imid, ihigh], axis=1)], axis=0)
    wide = jnp.dot(jnp.concatenate([high, mid], axis=1), both, preferred_element_type=F32)
    thin = jnp.dot(jnp.concatenate([high, low], axis=1), jnp.concatenate([ilow, ihigh], axis=0),
                   preferred_element_type=F32)
    v_ref[...] = wide[:, :k] + (wide[:, k:] + thin)


def solution(mesh):
    n = mesh.shape["rows"]
    m = mesh.shape["aux"]

    def shards(b, gaps, trial):
        rows, k = trial.shape
        pairs = b.shape[1]
        blk = 256
        steps = (rows + 2 * blk - 1) // (2 * blk)
        rows8 = (rows + 7) // 8 * 8
        dma = pltpu.SemaphoreType.DMA
        vmem = pl.BlockSpec(memory_space=pltpu.VMEM)
        anywhere = pl.BlockSpec(memory_space=pl.ANY)
        operands = [b]
        if rows % 8:
            operands.append(jnp.pad(b[(steps - 1) * 2 * blk:], ((0, -rows % 8), (0, 0))))
            trial = jnp.pad(trial, ((0, -rows % 8), (0, 0)))
        operands.append(trial)
        applied, inverse, rayleigh = pl.pallas_call(
            functools.partial(kernel, n, m, rows, ITERS),
            out_shape=(jax.ShapeDtypeStruct((rows8, k), F32),) + (jax.ShapeDtypeStruct((k, k), F32),) * 2,
            in_specs=[anywhere] * len(operands) + [vmem],
            out_specs=(anywhere, vmem, vmem),
            scratch_shapes=[
                pltpu.VMEM((2 * steps * blk, k), F32),
                pltpu.VMEM((2, 2 * blk, pairs), F32),
                pltpu.VMEM((2 * steps * blk, pairs), BF16),
                pltpu.VMEM((2 * steps * blk, pairs), BF16),
                pltpu.VMEM((pairs, 2 * k), BF16),
                pltpu.VMEM((steps, blk, k), F32),
                pltpu.VMEM((steps, blk, k), F32),
                pltpu.VMEM((steps, blk, k), F32),
                pltpu.VMEM((steps, blk, k), F32),
                pltpu.VMEM((2 * k, 2 * blk), BF16),
                pltpu.VMEM((k, pairs), F32),
                pltpu.VMEM((k, k), F32),
                pltpu.VMEM((k, pairs), F32),
                pltpu.VMEM((m - 1, k, pairs // m), F32),
                pltpu.VMEM((m, k, k), F32),
                pltpu.VMEM((k, k), F32),
                pltpu.VMEM((k, k), F32),
                pltpu.VMEM((k, k), F32),
                pltpu.VMEM((n - 1, k // n, k), F32),
                pltpu.VMEM((1, pairs), F32),
                dma((2,)), dma((1,)), dma((1,)),
            ] + [dma((ITERS, steps))] * 8 + [dma((ITERS + 1, m - 1))] * 6 + [dma((n - 1,))] * 4,
            compiler_params=pltpu.CompilerParams(collective_id=0, has_side_effects=True,
                                                 vmem_limit_bytes=63 * 1024 * 1024),
            name="subspace",
        )(*operands, gaps[None, :])
        tall = steps * blk
        vectors = pl.pallas_call(
            rotate_kernel,
            grid=((rows + tall - 1) // tall,),
            out_shape=jax.ShapeDtypeStruct((rows, k), F32),
            in_specs=[pl.BlockSpec((tall, k), lambda i: (i, 0)), pl.BlockSpec((k, k), lambda i: (0, 0))],
            out_specs=pl.BlockSpec((tall, k), lambda i: (i, 0)),
            name="rotate",
        )(applied, inverse)
        return vectors, rayleigh

    in_specs = (P("aux", "rows"), P("rows"), P("aux", None))
    return jax.shard_map(shards, mesh=mesh, in_specs=in_specs, out_specs=(P("aux", None), P()), check_vma=False)
```

```python
import functools

import jax
import jax.numpy as jnp
from jax import lax
from jax.experimental import pallas as pl
from jax.experimental.pallas import tpu as pltpu
from jax.sharding import PartitionSpec as P

ITERS = 2
MESH = pl.DeviceIdType.MESH
F32 = jnp.float32
BF16 = jnp.bfloat16
HIGHEST = lax.Precision.HIGHEST


def split(x):
    hi = x.astype(BF16)
    return hi, (x - hi.astype(F32)).astype(BF16)


def kernel(n, m, rows, iters, b_ref, *refs):
    if rows % 8:
        tail_ref, *refs = refs
    else:
        tail_ref = None
    (t_ref, gap_ref, v_ref, i_ref, r_ref, a_ref, bbuf, bhi, blo, s2, own, give, pair, came, cat, y_ref, c_ref,
     whole, got, grams, left, inv, part, gotr, w_ref,
     b_sem, t_sem, v_sem, pair_send, pair_recv, line_send, line_recv, back_send, back_recv, fwd_send, fwd_recv,
     rs_send, rs_recv, ag_send, ag_recv, g_send, g_recv, r_send, r_recv, q_send, q_recv) = refs
    h = n // 2
    me, mine = lax.axis_index("rows"), lax.axis_index("aux")
    z, c = me // 2, lax.rem(me, 2)
    at = z + c * (h - 1 - 2 * z)
    step_to = 1 - 2 * c
    steps, blk, k = own.shape
    pairs = bhi.shape[1]
    width = pairs // m
    last = rows - (steps - 1) * 2 * blk
    last8 = (last + 7) // 8 * 8
    rows8 = (rows + 7) // 8 * 8
    partner = {"rows": z * 2 + 1 - c}
    following = {"rows": (z + step_to) * 2 + c}
    previous = {"rows": (z - step_to) * 2 + c}
    first, end = at == 0, at == h - 1
    lag, ahead, behind = 6, 4, 6
    delay = 1 + ahead * at
    back = behind * (h - 1 - at) + lag
    across = behind // 2 * (h - 1) + lag

    def remote(src, dst, send, recv, to):
        return pltpu.make_async_remote_copy(src, dst, send, recv, device_id=to, device_id_type=MESH)

    def chunk(j):
        return pl.ds(pl.multiple_of(j * blk, blk), blk)

    def column(i):
        return pl.ds(pl.multiple_of(i * width, 128), width)

    def peer(d):
        return {"aux": lax.rem(mine + d, m)}

    barrier = pltpu.get_barrier_semaphore()
    for d in range(1, n):
        pl.semaphore_signal(barrier, inc=1, device_id={"rows": lax.rem(me + d, n)}, device_id_type=MESH)
    for d in range(1, m):
        pl.semaphore_signal(barrier, inc=1, device_id=peer(d), device_id_type=MESH)

    def full(i):
        return pltpu.make_async_copy(b_ref.at[pl.ds(pl.multiple_of(i * 2 * blk, 2 * blk), 2 * blk)],
                                     bbuf.at[lax.rem(i, 2)], b_sem.at[lax.rem(i, 2)])

    def short():
        src = tail_ref if rows % 8 else b_ref.at[pl.ds((steps - 1) * 2 * blk, last8)]
        slot = (steps - 1) % 2
        return pltpu.make_async_copy(src, bbuf.at[slot, pl.ds(0, last8)], b_sem.at[slot])

    def start(i):
        @pl.when(i < steps - 1)
        def _():
            full(i).start()

        @pl.when(i == steps - 1)
        def _():
            short().start()

    trial = pltpu.make_async_copy(t_ref, a_ref.at[pl.ds(0, rows8)], t_sem.at[0])
    trial.start()
    start(jnp.int32(0))
    start(jnp.int32(1))
    if rows8 < 2 * steps * blk:
        a_ref[pl.ds(rows8, 2 * steps * blk - rows8), :] = jnp.zeros((2 * steps * blk - rows8, k), F32)
    y_ref[...] = jnp.zeros_like(y_ref)
    gap = gap_ref[...]
    w_ref[...] = 4.0 * gap / (gap * gap + 1.0)
    trial.wait()

    def project(at_row, size, with_gram):
        where = pl.ds(pl.multiple_of(at_row, blk), size)
        a = a_ref[where, :]
        turned = a.T
        if with_gram:
            c_ref[...] += lax.dot_general(turned, a, (((1,), (0,)), ((), ())), precision=HIGHEST,
                                          preferred_element_type=F32)
        high, low = split(turned)
        cat[:k, :size] = high
        cat[k:, :size] = low
        for t in range(pairs // 256):
            cols = pl.ds(t * 256, 256)
            wide = jnp.dot(cat[:, :size], bhi[where, cols], preferred_element_type=F32)
            thin = jnp.dot(cat[:k, :size], blo[where, cols], preferred_element_type=F32)
            y_ref[:, cols] += wide[:k] + (wide[k:] + thin)

    def load(i, carry):
        @pl.when(i < steps - 1)
        def _():
            full(i).wait()

        @pl.when(i == steps - 1)
        def _():
            short().wait()
            if last8 < 2 * blk:
                bbuf[(steps - 1) % 2, pl.ds(last8, 2 * blk - last8), :] = jnp.zeros((2 * blk - last8, pairs), F32)

        for half in range(2):
            high, low = split(bbuf[lax.rem(i, 2), pl.ds(half * blk, blk), :])
            bhi[chunk(2 * i + half), :] = high
            blo[chunk(2 * i + half), :] = low
        start(i + 2)
        project(2 * i * blk, 2 * blk, False)
        return carry

    lax.fori_loop(0, steps, load, 0)
    pl.semaphore_wait(barrier, n - 1 + m - 1)

    group = 8

    def eliminate(tiles):
        def clear(g, carry):
            j = g * group
            u = [jnp.broadcast_to(left[pl.ds(j + q, 1), :], (8, k)) for q in range(group)]
            v = [jnp.broadcast_to(inv[pl.ds(j + q, 1), :], (8, k)) for q in range(group)]
            small = [[jnp.broadcast_to(u[q][:, p:p + 1], (8, k)) for p in range(group)] for q in range(group)]
            over = []
            for p in range(group):
                over.append(1.0 / small[p][p])
                for q in range(p + 1, group):
                    f = small[q][p] * over[p]
                    u[q] = u[q] - f * u[p]
                    v[q] = v[q] - f * v[p]
                    for r in range(p + 1, group):
                        small[q][r] = small[q][r] - f * small[p][r]
            kept = [v[q] / jnp.sqrt(small[q][q]) for q in range(group)]
            for p in reversed(range(group)):
                for q in range(p + 1, group):
                    u[p] = u[p] - small[p][q] * u[q]
                    v[p] = v[p] - small[p][q] * v[q]
                u[p] = u[p] * over[p]
                v[p] = v[p] * over[p]
            for t in tiles:
                tile = pl.ds(t * 8, 8)
                a, x = left[tile, :], inv[tile, :]
                below = lax.broadcasted_iota(jnp.int32, (8, k), 0) + t * 8 >= j + group
                for q in range(group):
                    f = jnp.where(below, left[tile, q:q + 1], 0.0)
                    a = a - f * u[q]
                    x = x - f * v[q]
                left[tile, :] = pltpu.roll(a, k - group, 1)
                inv[tile, :] = x
            for q in range(group):
                inv[pl.ds(j + q, 1), :] = kept[q][:1]
            return carry

        return clear

    def between(e):
        def gram(d, whose):
            return remote(c_ref, grams.at[whose], g_send.at[e, d - 1], g_recv.at[e, d - 1], peer(d))

        def scatter(d):
            return remote(y_ref.at[:, column(lax.rem(mine + d, m))], got.at[d - 1],
                          rs_send.at[e, d - 1], rs_recv.at[e, d - 1], peer(d))

        def gather(d, whose):
            return remote(whole.at[:, column(whose)], whole.at[:, column(whose)],
                          ag_send.at[e, d - 1], ag_recv.at[e, d - 1], peer(d))

        if e:
            for d in range(1, m):
                gram(d, mine).start()
        for d in range(1, m):
            scatter(d).start()

        def sums():
            total = y_ref[:, column(mine)]
            for d in range(1, m):
                scatter(d).wait_recv()
                total = total + got[d - 1]
            whole[:, column(mine)] = total
            if e < iters:
                for d in range(1, m):
                    gather(d, mine).start()

        if e:
            grams[mine] = c_ref[...]
            for d in range(1, m):
                gram(d, lax.rem(mine + m - d, m)).wait_recv()
            total = grams[0]
            for i in range(1, m):
                total = total + grams[i]
            left[...] = total
            inv[...] = (lax.broadcasted_iota(jnp.int32, (k, k), 0)
                        == lax.broadcasted_iota(jnp.int32, (k, k), 1)).astype(F32)
            lax.fori_loop(0, k // group // 2, eliminate(range(k // 8)), 0)
            sums()
            lax.fori_loop(k // group // 2, k // group, eliminate(range(k // 16, k // 8)), 0)
        else:
            sums()
        if e == iters:
            pt = jnp.dot(inv[...], whole[:, column(mine)], precision=HIGHEST, preferred_element_type=F32)
            part[...] = lax.dot_general(pt, pt * w_ref[:, column(mine)], (((1,), (1,)), ((), ())),
                                        precision=HIGHEST, preferred_element_type=F32)
            for d in range(1, m):
                gram(d, mine).wait_send()
                scatter(d).wait_send()
            return
        for d in range(1, m):
            gather(d, lax.rem(mine + m - d, m)).wait_recv()
        for t in range(pairs // 256):
            cols = pl.ds(t * 256, 256)
            pt = whole[:, cols]
            if e:
                pt = jnp.dot(inv[...], pt, precision=HIGHEST, preferred_element_type=F32)
            scaled = pt * w_ref[:, cols]
            high, low = split(scaled.T)
            s2[cols, :k] = high
            s2[cols, k:] = low
        for d in range(1, m):
            if e:
                gram(d, mine).wait_send()
            scatter(d).wait_send()
            gather(d, mine).wait_send()

    def line(e):
        def over(i):
            return remote(give.at[i], pair.at[i], pair_send.at[e, i], pair_recv.at[e, i], partner)

        def onward(i):
            return remote(own.at[i], came.at[i], line_send.at[e, i], line_recv.at[e, i], following)

        def backward(i):
            return remote(a_ref.at[chunk(2 * i + c)], a_ref.at[chunk(2 * i + c)],
                          back_send.at[e, i], back_recv.at[e, i], previous)

        def share(i, j):
            return remote(a_ref.at[chunk(j)], a_ref.at[chunk(j)], fwd_send.at[e, i], fwd_recv.at[e, i], partner)

        def product(j):
            wide = jnp.dot(bhi[chunk(j), :], s2[...], preferred_element_type=F32)
            thin = jnp.dot(blo[chunk(j), :], s2[:, :k], preferred_element_type=F32)
            return wide[:, :k] + (wide[:, k:] + thin)

        def multiply(i):
            give[i] = product(2 * i + 1 - c)
            over(i).start()
            own[i] = product(2 * i + c)

        def reduce(i):
            over(i).wait_recv()
            own[i] = own[i] + pair[i]

            @pl.when(jnp.logical_not(first))
            def _():
                onward(i).wait_recv()
                own[i] = own[i] + came[i]

            @pl.when(jnp.logical_not(end))
            def _():
                onward(i).start()

            @pl.when(end)
            def _():
                a_ref[chunk(2 * i + c), :] = own[i]

        y_ref[...] = jnp.zeros_like(y_ref)
        c_ref[...] = jnp.zeros_like(c_ref)

        def step(t, carry):
            @pl.when(t < steps)
            def _():
                multiply(t)

            i = t - delay

            @pl.when(jnp.logical_and(i >= 0, i < steps))
            def _():
                reduce(i)

            i = t - delay - back

            @pl.when(jnp.logical_and(i >= 0, i < steps))
            def _():
                @pl.when(jnp.logical_not(end))
                def _():
                    backward(i).wait_recv()

                @pl.when(jnp.logical_not(first))
                def _():
                    backward(i).start()

                share(i, 2 * i + c).start()
                project((2 * i + c) * blk, blk, True)

            i = t - delay - across

            @pl.when(jnp.logical_and(i >= 0, i < steps))
            def _():
                share(i, 2 * i + 1 - c).wait_recv()
                project((2 * i + 1 - c) * blk, blk, True)

            return carry

        lax.fori_loop(0, steps + 1 + (ahead + behind) * (h - 1) + lag, step, 0)

        def drain(i, carry):
            over(i).wait_send()
            share(i, 2 * i + c).wait_send()

            @pl.when(jnp.logical_not(end))
            def _():
                onward(i).wait_send()

            @pl.when(jnp.logical_not(first))
            def _():
                backward(i).wait_send()

            return carry

        lax.fori_loop(0, steps, drain, 0)

    between(0)
    for e in range(iters):
        line(e)
        if e == iters - 1:
            done = pltpu.make_async_copy(a_ref.at[pl.ds(0, rows8)], v_ref, v_sem.at[0])
            done.start()
        between(e + 1)
    i_ref[...] = inv[...]

    slab = k // n

    def strip(i):
        return pl.ds(pl.multiple_of(i * slab, 8), slab)

    def scatter(d):
        to = lax.rem(me + d, n)
        return remote(part.at[strip(to)], gotr.at[d - 1], r_send.at[d - 1], r_recv.at[d - 1], {"rows": to})

    def gather(d, whose):
        return remote(r_ref.at[strip(whose)], r_ref.at[strip(whose)], q_send.at[d - 1], q_recv.at[d - 1],
                      {"rows": lax.rem(me + d, n)})

    for d in range(1, n):
        scatter(d).start()

    total = part[strip(me), :]
    for d in range(1, n):
        scatter(d).wait_recv()
        total = total + gotr[d - 1]

    def spread(d, whose):
        return remote(pair.at[whose, pl.ds(0, slab)], pair.at[whose, pl.ds(0, slab)],
                      ag_send.at[iters, d - 1], ag_recv.at[iters, d - 1], peer(d))

    pair[mine, pl.ds(0, slab), :] = total
    for d in range(1, m):
        spread(d, mine).start()
    for d in range(1, m):
        spread(d, lax.rem(mine + m - d, m)).wait_recv()
    total = pair[0, pl.ds(0, slab), :]
    for i in range(1, m):
        total = total + pair[i, pl.ds(0, slab), :]
    for d in range(1, m):
        spread(d, mine).wait_send()
    r_ref[strip(me), :] = total
    for d in range(1, n):
        gather(d, me).start()
    for d in range(1, n):
        gather(d, lax.rem(me + n - d, n)).wait_recv()
    for d in range(1, n):
        scatter(d).wait_send()
        gather(d, me).wait_send()
    done.wait()


def rotate_kernel(a_ref, i_ref, v_ref):
    def thirds(x):
        high, rest = x.astype(BF16), x - x.astype(BF16).astype(F32)
        return (high,) + split(rest)

    high, mid, low = thirds(a_ref[...])
    ihigh, imid, ilow = thirds(i_ref[...].T)
    k = ihigh.shape[1]
    both = jnp.concatenate([jnp.concatenate([ihigh, imid], axis=1), jnp.concatenate([imid, ihigh], axis=1)], axis=0)
    wide = jnp.dot(jnp.concatenate([high, mid], axis=1), both, preferred_element_type=F32)
    thin = jnp.dot(jnp.concatenate([high, low], axis=1), jnp.concatenate([ilow, ihigh], axis=0),
                   preferred_element_type=F32)
    v_ref[...] = wide[:, :k] + (wide[:, k:] + thin)


def solution(mesh):
    n = mesh.shape["rows"]
    m = mesh.shape["aux"]

    def shards(b, gaps, trial):
        rows, k = trial.shape
        pairs = b.shape[1]
        blk = 256
        steps = (rows + 2 * blk - 1) // (2 * blk)
        rows8 = (rows + 7) // 8 * 8
        dma = pltpu.SemaphoreType.DMA
        vmem = pl.BlockSpec(memory_space=pltpu.VMEM)
        anywhere = pl.BlockSpec(memory_space=pl.ANY)
        operands = [b]
        if rows % 8:
            operands.append(jnp.pad(b[(steps - 1) * 2 * blk:], ((0, -rows % 8), (0, 0))))
            trial = jnp.pad(trial, ((0, -rows % 8), (0, 0)))
        operands.append(trial)
        applied, inverse, rayleigh = pl.pallas_call(
            functools.partial(kernel, n, m, rows, ITERS),
            out_shape=(jax.ShapeDtypeStruct((rows8, k), F32),) + (jax.ShapeDtypeStruct((k, k), F32),) * 2,
            in_specs=[anywhere] * len(operands) + [vmem],
            out_specs=(anywhere, vmem, vmem),
            scratch_shapes=[
                pltpu.VMEM((2 * steps * blk, k), F32),
                pltpu.VMEM((2, 2 * blk, pairs), F32),
                pltpu.VMEM((2 * steps * blk, pairs), BF16),
                pltpu.VMEM((2 * steps * blk, pairs), BF16),
                pltpu.VMEM((pairs, 2 * k), BF16),
                pltpu.VMEM((steps, blk, k), F32),
                pltpu.VMEM((steps, blk, k), F32),
                pltpu.VMEM((steps, blk, k), F32),
                pltpu.VMEM((steps, blk, k), F32),
                pltpu.VMEM((2 * k, 2 * blk), BF16),
                pltpu.VMEM((k, pairs), F32),
                pltpu.VMEM((k, k), F32),
                pltpu.VMEM((k, pairs), F32),
                pltpu.VMEM((m - 1, k, pairs // m), F32),
                pltpu.VMEM((m, k, k), F32),
                pltpu.VMEM((k, k), F32),
                pltpu.VMEM((k, k), F32),
                pltpu.VMEM((k, k), F32),
                pltpu.VMEM((n - 1, k // n, k), F32),
                pltpu.VMEM((1, pairs), F32),
                dma((2,)), dma((1,)), dma((1,)),
            ] + [dma((ITERS, steps))] * 8 + [dma((ITERS + 1, m - 1))] * 6 + [dma((n - 1,))] * 4,
            compiler_params=pltpu.CompilerParams(collective_id=0, has_side_effects=True,
                                                 vmem_limit_bytes=63 * 1024 * 1024),
            name="subspace",
        )(*operands, gaps[None, :])
        tall = steps * blk
        vectors = pl.pallas_call(
            rotate_kernel,
            grid=((rows + tall - 1) // tall,),
            out_shape=jax.ShapeDtypeStruct((rows, k), F32),
            in_specs=[pl.BlockSpec((tall, k), lambda i: (i, 0)), pl.BlockSpec((k, k), lambda i: (0, 0))],
            out_specs=pl.BlockSpec((tall, k), lambda i: (i, 0)),
            name="rotate",
        )(applied, inverse)
        return vectors, rayleigh

    in_specs = (P("aux", "rows"), P("rows"), P("aux", None))
    return jax.shard_map(shards, mesh=mesh, in_specs=in_specs, out_specs=(P("aux", None), P()), check_vma=False)
```
